32 devices in a mesh: dom: 16 (over z, y, x), grp: 2 (over core).
Axes of the slice: x: 2, y: 2, z: 4, core: 2. Of those that a mesh axis runs over, the one named last changes fastest.
Arguments:
- node_features: bfloat16 [262144, 256], P(('dom', 'grp')), may hold values from -6 to 6
- vertex_count: int32 [32], P(('dom', 'grp')), may hold values from 4096 to 8192, as said below
- send_rows: int32 [32, 2, 2048], P(('dom', 'grp')), may hold values from 0 to 8191, as said below
- block_values: bfloat16 [2048, 4, 128, 128], P(('dom', 'grp')), may hold values from -0.25 to 0.25
- block_cols: int32 [2048, 4], P(('dom', 'grp')), may hold values from 0 to 95
- block_count: int32 [2048], P(('dom', 'grp')), may hold values from 1 to 4
- w_query: bfloat16 [2, 256, 256], replicated, may hold values from -0.375 to 0.375
- w_key: bfloat16 [2, 256, 256], replicated, may hold values from -0.375 to 0.375
- w_value: bfloat16 [2, 256, 256], replicated, may hold values from -0.375 to 0.375
- w_message: bfloat16 [2, 256, 256], replicated, may hold values from -0.375 to 0.375
- w_out: bfloat16 [2, 256, 256], replicated, may hold values from -0.375 to 0.375
- attn_gain: float32 [2, 256], replicated, may hold values from 0.25 to 1.75
Outputs:
- updated: bfloat16 [262144, 256], P(('dom', 'grp'))
The draws below stay inside these ranges and needn't reach their ends.
Inputs may be any that keep to these rules, and one draw needn't show every extreme that they name: Rows of partition p at local index vertex_count[p] or above are padding; some partition uses all 8192 slots. send_rows[p, 0, :] and send_rows[p, 1, :] each list 2048 distinct local rows of partition p below vertex_count[p]. `block_cols`: extended tiles below 64 are the partition's own; the next 16 come from the lower neighbour, the last 16 from the upper one. Only the first block_count[g] blocks of row tile g are used.
All inputs are finite; a program needn't handle non-finite values.
Results may differ from the reference program's by a relative error of at most 0.0063.
Values may be sent and summed in bfloat16 or wider, within the bound.
A program may use at most 128 MiB of HBM per device.

```python
import jax
import jax.numpy as jnp
from jax import lax

D = 256
TILE = 128
NB = 4
LAYERS = 2
V_DEV = 8192
HALO = 2048
TILES_DEV = 64
EXT_TILES = 96
PARTITIONS = 32
VERTICES = 262144
ALL_TILES = 2048


def count_draw(key):
    counts = jax.random.randint(jax.random.fold_in(key, 11), (PARTITIONS,), V_DEV // 2, V_DEV + 1)
    chosen = jax.random.randint(jax.random.fold_in(key, 12), (), 0, PARTITIONS)
    counts = jnp.where(jnp.arange(PARTITIONS) == chosen, V_DEV, counts)
    return counts.astype(jnp.int32)


def draw_vertex_count(key, part):
    return count_draw(key)


def draw_send_rows(key, part):
    counts = count_draw(key)
    scores = jax.random.randint(jax.random.fold_in(key, 13), (PARTITIONS, 2, V_DEV), 0, 1048576)
    row_index = jnp.arange(V_DEV, dtype=jnp.int32)
    beyond = row_index[None, None, :] >= counts[:, None, None]
    scores = scores + jnp.where(beyond, 2097152, 0)
    order = jnp.argsort(scores, axis=-1, stable=True)
    return order[:, :, :HALO].astype(jnp.int32)


def with_ends(drawn, key, smallest, top_value):
    index_at = [jax.random.randint(jax.random.fold_in(key, axis), (), 0, length) for axis, length in enumerate(drawn.shape)]
    widest = drawn.shape.index(max(drawn.shape))
    next_to = index_at[:widest] + [(index_at[widest] + 1) % drawn.shape[widest]] + index_at[widest + 1:]
    return drawn.at[tuple(index_at)].set(smallest).at[tuple(next_to)].set(top_value)


def block_scale(rng, shape, pieces, low, largest):
    gain = 1.0
    for dim, shards_of in pieces:
        draws = jax.random.uniform(jax.random.fold_in(jax.random.fold_in(rng, 6), dim), (shards_of,), jnp.float32, low / len(pieces), largest / len(pieces))
        gain = gain * jnp.repeat(jnp.exp(draws), shape[dim] // shards_of).reshape((-1,) + (1,) * (len(shape) - 1 - dim))
    return gain


def centred(own_key, shape, scale, most, split=(), held_as=jnp.bfloat16):
    drawn = scale * jax.random.normal(own_key, shape, jnp.float32)
    if split:
        drawn = drawn * block_scale(own_key, shape, split, -0.22, 0.18)
    return jnp.clip(drawn, -most, most).astype(held_as)


def setup_inputs(seed: int = 0) -> dict:
    splits = jax.random.split(jax.random.key(seed), 13)
    node_features = centred(splits[0], (VERTICES, D), 1.0, 6.0, ((0, 32),))
    vertex_count = draw_vertex_count(jax.random.fold_in(splits[12], 71), 0)
    send_rows = draw_send_rows(jax.random.fold_in(splits[12], 71), 0)
    block_values = centred(splits[3], (ALL_TILES, NB, TILE, TILE), (NB * TILE) ** -0.5, 0.25, ((0, 32),))
    block_cols = with_ends(jax.random.randint(splits[4], (ALL_TILES, NB), 0, EXT_TILES), jax.random.fold_in(splits[4], 1), 0, EXT_TILES - 1).astype(jnp.int32)
    block_count = with_ends(jax.random.randint(splits[5], (ALL_TILES,), 1, NB + 1), jax.random.fold_in(splits[5], 1), 1, NB).astype(jnp.int32)
    w_query = centred(splits[6], (LAYERS, D, D), D ** -0.5, 0.375)
    w_key = centred(splits[7], (LAYERS, D, D), D ** -0.5, 0.375)
    w_value = centred(splits[8], (LAYERS, D, D), D ** -0.5, 0.375)
    w_message = centred(splits[9], (LAYERS, D, D), D ** -0.5, 0.375)
    w_out = centred(splits[10], (LAYERS, D, D), D ** -0.5, 0.375)
    attn_gain = jnp.clip(1.0 + 0.15 * jax.random.normal(splits[11], (LAYERS, D), jnp.float32), 0.25, 1.75)
    return dict(node_features=node_features, vertex_count=vertex_count, send_rows=send_rows, block_values=block_values, block_cols=block_cols, block_count=block_count, w_query=w_query, w_key=w_key, w_value=w_value, w_message=w_message, w_out=w_out, attn_gain=attn_gain)


epsilon = 1e-06

def feature_map(inputs):
    return jax.nn.elu(inputs) + 1.0

def reference(node_features, vertex_count, send_rows, block_values, block_cols, block_count, w_query, w_key, w_value, w_message, w_out, attn_gain):
    row_index = jnp.arange(V_DEV, dtype=jnp.int32)
    valid_rows = (row_index[None, :] < vertex_count[:, None]).astype(jnp.float32)
    hidden = node_features.reshape(PARTITIONS, V_DEV, D)
    hidden = jnp.where(valid_rows[..., None] > 0.5, hidden, jnp.zeros_like(hidden))
    tile_blocks = block_values.reshape(PARTITIONS, TILES_DEV, NB, TILE, TILE)
    tile_cols = block_cols.reshape(PARTITIONS, TILES_DEV, NB)
    tile_counts = block_count.reshape(PARTITIONS, TILES_DEV)
    for layer_num in range(LAYERS):

        def add_summary(running, entries):
            part_rows, keep_rows = entries
            key_rows = (feature_map(jnp.dot(part_rows, w_key[layer_num], preferred_element_type=jnp.float32)) * keep_rows[:, None]).astype(jnp.bfloat16)
            value_rows = jnp.dot(part_rows, w_value[layer_num], preferred_element_type=jnp.float32).astype(jnp.bfloat16)
            return (running + jnp.dot(key_rows.T, value_rows, preferred_element_type=jnp.float32), None)
        summary, _ = lax.scan(add_summary, jnp.zeros((D, D), jnp.float32), (hidden, valid_rows))
        summary_cast = summary.astype(jnp.bfloat16)
        outgoing = jax.vmap(lambda part_rows, row_list: part_rows[row_list])(hidden, send_rows)
        zero_rows = jnp.zeros((1, HALO, D), jnp.bfloat16)
        lower_rows = jnp.concatenate([zero_rows, outgoing[:-1, 1]], axis=0)
        upper_rows = jnp.concatenate([outgoing[1:, 0], zero_rows], axis=0)

        def update(entries):
            part_rows, keep_rows, below, above, blocks_here, cols_here, counts_here = entries
            extended = jnp.concatenate([part_rows, below, above], axis=0).reshape(EXT_TILES, TILE, D)
            picked = extended[cols_here]
            live_slots = jnp.arange(NB, dtype=jnp.int32)[None, :] < counts_here[:, None]
            used_blocks = jnp.where(live_slots[:, :, None, None], blocks_here, jnp.zeros_like(blocks_here))
            aggregated = jnp.einsum('tjab,tjbd->tad', used_blocks.astype(jnp.float32), picked.astype(jnp.float32))
            aggregated = aggregated.reshape(V_DEV, D).astype(jnp.bfloat16)
            message = jax.nn.silu(jnp.dot(aggregated, w_message[layer_num], preferred_element_type=jnp.float32))
            query_rows = feature_map(jnp.dot(part_rows, w_query[layer_num], preferred_element_type=jnp.float32)).astype(jnp.bfloat16)
            mixed_rows = jnp.dot(query_rows, summary_cast, preferred_element_type=jnp.float32)
            scale = lax.rsqrt(lax.optimization_barrier(jnp.mean(mixed_rows * mixed_rows, axis=-1, keepdims=True)) + epsilon)
            attended = (mixed_rows * scale * attn_gain[layer_num][None, :]).astype(jnp.bfloat16)
            output = jnp.dot(attended, w_out[layer_num], preferred_element_type=jnp.float32)
            renewed = part_rows.astype(jnp.float32) + message + output
            renewed = jnp.where(keep_rows[:, None] > 0.5, renewed, jnp.zeros_like(renewed))
            return renewed.astype(jnp.bfloat16)
        hidden = lax.map(update, (hidden, valid_rows, lower_rows, upper_rows, tile_blocks, tile_cols, tile_counts))
    return hidden.reshape(VERTICES, D)
```

```python
import functools

import jax
import jax.numpy as jnp
from jax import lax
from jax.experimental import pallas as pl
from jax.experimental.pallas import tpu as pltpu
from jax.sharding import PartitionSpec as P

EPSILON = 1e-06
MESH = pl.DeviceIdType.MESH
ROWS = 1024
LOAD_PIECES = 8


def feature_map(u):
    return jnp.where(u > 0, u + 1.0, jnp.exp(u))


def silu(u):
    half = 0.5 * u
    return half * (1.0 + jnp.tanh(half))


def dot(a, b):
    return jnp.dot(a, b, preferred_element_type=jnp.float32)


def kernel(
    axes,
    sizes,
    count_ref,
    send_ref,
    cols_ref,
    used_ref,
    nodes_ref,
    blocks_ref,
    wq_ref,
    wk_ref,
    wv_ref,
    wm_ref,
    wo_ref,
    gain_ref,
    out_ref,
    blocks,
    pairs,
    picked,
    outgoing,
    query,
    base,
    partial,
    shards,
    summary,
    load_sem,
    block_sem,
    store_sem,
    halo_send,
    halo_recv,
    rs_send,
    rs_recv,
    ag_send,
    ag_recv,
    *ext,
):
    layers = wq_ref.shape[0]
    tile, width = nodes_ref.shape[1:]
    vertices = nodes_ref.shape[0] * tile
    half = width // 2
    slots = blocks.shape[1]
    halo = outgoing.shape[1] * tile
    shard = shards.shape[2]
    owners = width // shard
    total = sizes[0] * sizes[1]
    me = lax.axis_index(axes[0]) * sizes[1] + lax.axis_index(axes[1])

    def device(index):
        return (index // sizes[1], index % sizes[1])

    def others(body):
        def step(k, carry):
            body(k)
            return carry

        lax.fori_loop(1, total, step, 0)

    def when(needed, condition, body):
        if needed:
            pl.when(condition)(body)
        else:
            body()

    barrier = pltpu.get_barrier_semaphore()
    others(
        lambda k: pl.semaphore_signal(
            barrier, inc=1, device_id=device((me + k) % total), device_id_type=MESH
        )
    )

    block_copy = pltpu.make_async_copy(blocks_ref, blocks, block_sem)
    piece = vertices // LOAD_PIECES
    loads = [
        pltpu.make_async_copy(
            nodes_ref.at[pl.ds(i * piece // tile, piece // tile)],
            ext[0].at[pl.ds(i * piece // tile, piece // tile)],
            load_sem.at[i],
        )
        for i in range(LOAD_PIECES)
    ]
    for load in loads:
        load.start()
    block_copy.start()

    valid = count_ref[0]

    def row_mask(start, rows):
        index = lax.broadcasted_iota(jnp.int32, (rows, width), 0) + start
        return index < valid

    def own_rows_of(layer, start):
        return ext[layer][pl.ds(start // tile, ROWS // tile)].reshape(ROWS, width)

    def keep_own_rows(layer, start, value):
        ext[layer][pl.ds(start // tile, ROWS // tile)] = value.reshape(ROWS // tile, tile, width)

    def keep_pairs(start, value):
        pairs[0, pl.ds(start, ROWS), :] = value[:, :half]
        pairs[1, pl.ds(start, ROWS), :] = value[:, half:]

    def chunks(body, first, last):
        def step(i, carry):
            body(pl.multiple_of(i * ROWS, ROWS))
            return carry

        lax.fori_loop(first, last, step, 0)

    per_piece = piece // ROWS
    for i in range(LOAD_PIECES):
        loads[i].wait()

        def clean(start):
            rows = own_rows_of(0, start).astype(jnp.float32)
            rows = jnp.where(row_mask(start, ROWS), rows, 0.0)
            keep_own_rows(0, start, rows.astype(jnp.bfloat16))
            keep_pairs(start, rows)

        chunks(clean, i * per_piece, (i + 1) * per_piece)

    for layer in range(layers):

        @pl.when(me == 0)
        def _():
            ext[layer][pl.ds(vertices // tile, halo // tile)] = jnp.zeros(outgoing.shape[1:], jnp.bfloat16)

        @pl.when(me == total - 1)
        def _():
            ext[layer][pl.ds((vertices + halo) // tile, halo // tile)] = jnp.zeros(outgoing.shape[1:], jnp.bfloat16)

    pl.semaphore_wait(barrier, total - 1)

    pieces = vertices // ROWS
    send_rows = halo // pieces

    def halo_copy(layer, side, part):
        target = me + (1 if side else -1)
        where = vertices + (0 if side else halo) + part * send_rows
        return pltpu.make_async_remote_copy(
            src_ref=outgoing.at[side, pl.ds(part * send_rows // tile, send_rows // tile)],
            dst_ref=ext[layer].at[pl.ds(where // tile, send_rows // tile)],
            send_sem=halo_send.at[layer, side, part],
            recv_sem=halo_recv.at[layer, side, part],
            device_id=device(target),
            device_id_type=MESH,
        )

    def sends_to(side):
        return me < total - 1 if side else me > 0

    def gets_from(side):
        return me > 0 if side else me < total - 1

    def halo_each(layer, wanted, act):
        for side in range(2):

            @pl.when(wanted(side))
            def _():
                def step(part, carry):
                    act(halo_copy(layer, side, part))
                    return carry

                lax.fori_loop(0, pieces, step, 0)

    def shard_copy(layer, k):
        target = (me + k) % total
        return pltpu.make_async_remote_copy(
            src_ref=partial.at[pl.ds(pl.multiple_of(target % owners * shard, shard), shard)],
            dst_ref=shards.at[layer, k],
            send_sem=rs_send.at[k],
            recv_sem=rs_recv.at[layer, k],
            device_id=device(target),
            device_id_type=MESH,
        )

    def summary_copy(layer, k, owner):
        rows = pl.ds(pl.multiple_of(owner % owners * shard, shard), shard)
        return pltpu.make_async_remote_copy(
            src_ref=summary.at[layer, rows],
            dst_ref=summary.at[layer, rows],
            send_sem=ag_send.at[layer, k],
            recv_sem=ag_recv.at[layer, k],
            device_id=device((me + k) % total),
            device_id_type=MESH,
        )

    extra = total > owners
    own_rows = pl.ds(pl.multiple_of(me % owners * shard, shard), shard)

    for layer in range(layers):
        last = layer == layers - 1
        if layer:
            halo_each(layer - 1, sends_to, lambda copy: copy.wait_send())

        if layer:
            others(
                lambda k: when(
                    extra,
                    (me + k) % total < owners,
                    lambda: shard_copy(layer - 1, k).wait_send(),
                )
            )
        partial[...] = jnp.zeros_like(partial)

        def key_value(start):
            rows = own_rows_of(layer, start)
            keys = feature_map(dot(rows, wk_ref[layer]))
            keys = jnp.where(row_mask(start, ROWS), keys, 0.0).astype(jnp.bfloat16)
            values = dot(rows, wv_ref[layer]).astype(jnp.bfloat16)
            partial[...] += lax.dot_general(
                keys, values, (((0,), (0,)), ((), ())), preferred_element_type=jnp.float32
            )
            part = start // ROWS
            for side in range(2):
                for u in range(send_rows):
                    row = send_ref[0, side, part * send_rows + u]
                    for h in range(2):
                        picked[side, h, u] = pairs[h, row]
                for h in range(2):
                    outgoing[
                        side,
                        pl.ds(part * (send_rows // tile), send_rows // tile),
                        :,
                        h * half : (h + 1) * half,
                    ] = picked[side, h].astype(jnp.bfloat16).reshape(-1, tile, half)
            for side in range(2):

                @pl.when(sends_to(side))
                def _():
                    halo_copy(layer, side, part).start()

        chunks(key_value, 0, vertices // ROWS)

        others(
            lambda k: when(
                extra, (me + k) % total < owners, lambda: shard_copy(layer, k).start()
            )
        )

        def queries(start):
            rows = own_rows_of(layer, start)
            query[pl.ds(start, ROWS), :] = feature_map(dot(rows, wq_ref[layer])).astype(
                jnp.bfloat16
            )

        chunks(queries, 0, vertices // ROWS)

        def reduce_shard():
            others(lambda k: shard_copy(layer, k).wait_recv())
            reduced = lax.fori_loop(
                1, total, lambda k, acc: acc + shards[layer, k], partial[own_rows, :]
            )
            summary[layer, own_rows, :] = reduced
            others(lambda k: summary_copy(layer, k, me).start())

        when(extra, me < owners, reduce_shard)
        others(
            lambda k: when(
                extra,
                (me + total - k) % total < owners,
                lambda: summary_copy(layer, k, (me + total - k) % total).wait_recv(),
            )
        )

        def attend(start):
            mixed = dot(query[pl.ds(start, ROWS), :], summary[layer].astype(jnp.bfloat16))
            scale = lax.rsqrt(jnp.mean(mixed * mixed, axis=-1, keepdims=True) + EPSILON)
            attended = (mixed * scale * gain_ref[pl.ds(layer, 1), :]).astype(jnp.bfloat16)
            rows = own_rows_of(layer, start).astype(jnp.float32)
            base[pl.ds(start, ROWS), :] = rows + dot(attended, wo_ref[layer])

        chunks(attend, 0, vertices // ROWS)

        halo_each(layer, gets_from, lambda copy: copy.wait_recv())
        if not layer:
            block_copy.wait()

        slot_of_lane = lax.broadcasted_iota(jnp.int32, (1, slots * tile), 1) // tile

        def aggregate(start):
            parts = []
            for t in range(ROWS // tile):
                index = start // tile + t
                live = (slot_of_lane < used_ref[index]).astype(jnp.float32).astype(jnp.bfloat16)
                left, right = [], []
                for j in range(slots):
                    left.append(blocks[index, j])
                    right.append(ext[layer][cols_ref[index, j]])
                live_blocks = jnp.concatenate(left, axis=1) * live
                parts.append(dot(live_blocks, jnp.concatenate(right, axis=0)))
            aggregated = jnp.concatenate(parts, axis=0).astype(jnp.bfloat16)
            message = silu(dot(aggregated, wm_ref[layer]))
            renewed = base[pl.ds(start, ROWS), :] + message
            renewed = jnp.where(row_mask(start, ROWS), renewed, 0.0).astype(jnp.bfloat16)
            if last:
                query[pl.ds(start, ROWS), :] = renewed
                pltpu.make_async_copy(
                    query.at[pl.ds(start, ROWS)],
                    out_ref.at[pl.ds(start, ROWS)],
                    store_sem.at[start // ROWS],
                ).start()
            else:
                keep_own_rows(layer + 1, start, renewed)
                keep_pairs(start, renewed.astype(jnp.float32))

        chunks(aggregate, 0, vertices // ROWS)

        def sent():
            others(lambda k: summary_copy(layer, k, me).wait_send())

        when(extra, me < owners, sent)

    halo_each(layers - 1, sends_to, lambda copy: copy.wait_send())
    others(
        lambda k: when(
            extra, (me + k) % total < owners, lambda: shard_copy(layers - 1, k).wait_send()
        )
    )

    def stored(start):
        pltpu.make_async_copy(
            query.at[pl.ds(start, ROWS)],
            out_ref.at[pl.ds(start, ROWS)],
            store_sem.at[start // ROWS],
        ).wait()

    chunks(stored, 0, vertices // ROWS)


def solution(mesh):
    axes = tuple(mesh.axis_names)
    sizes = tuple(mesh.shape[a] for a in axes)
    total = sizes[0] * sizes[1]

    def on_device(
        node_features,
        vertex_count,
        send_rows,
        block_values,
        block_cols,
        block_count,
        w_query,
        w_key,
        w_value,
        w_message,
        w_out,
        attn_gain,
    ):
        vertices, width = node_features.shape
        layers = w_query.shape[0]
        halo = send_rows.shape[2]
        tile = block_values.shape[2]
        pieces = vertices // ROWS
        shard = max(8, width // total)
        bf16, f32, dma = jnp.bfloat16, jnp.float32, pltpu.SemaphoreType.DMA
        smem = pl.BlockSpec(memory_space=pltpu.SMEM)
        vmem = pl.BlockSpec(memory_space=pltpu.VMEM)
        anywhere = pl.BlockSpec(memory_space=pl.ANY)
        return pl.pallas_call(
            functools.partial(kernel, axes, sizes),
            name="graph_layers",
            out_shape=jax.ShapeDtypeStruct((vertices, width), bf16),
            in_specs=[smem] * 4 + [anywhere] * 2 + [vmem] * 6,
            out_specs=anywhere,
            scratch_shapes=[
                pltpu.VMEM(block_values.shape, bf16),
                pltpu.VMEM((2, vertices, width // 2), f32),
                pltpu.VMEM((2, 2, halo // pieces, width // 2), f32),
                pltpu.VMEM((2, halo // tile, tile, width), bf16),
                pltpu.VMEM((vertices, width), bf16),
                pltpu.VMEM((vertices, width), f32),
                pltpu.VMEM((width, width), f32),
                pltpu.VMEM((layers, total, shard, width), f32),
                pltpu.VMEM((layers, width, width), f32),
                dma((LOAD_PIECES,)),
                dma(()),
                dma((vertices // ROWS,)),
                dma((layers, 2, pieces)),
                dma((layers, 2, pieces)),
                dma((total,)),
                dma((layers, total)),
                dma((layers, total)),
                dma((layers, total)),
            ]
            + [pltpu.VMEM(((vertices + 2 * halo) // tile, tile, width), bf16)] * layers,
            compiler_params=pltpu.CompilerParams(
                collective_id=0, has_side_effects=True, vmem_limit_bytes=67043328
            ),
        )(
            vertex_count,
            send_rows,
            block_cols,
            block_count,
            node_features.reshape(-1, tile, width),
            block_values,
            w_query,
            w_key,
            w_value,
            w_message,
            w_out,
            attn_gain,
        )

    rows = P(axes, None)
    placed = (rows, P(axes), P(axes, None, None), P(axes, None, None, None), rows, P(axes))
    return jax.shard_map(
        on_device, mesh=mesh, in_specs=placed + (P(),) * 6, out_specs=rows, check_vma=False
    )
```
